32 devices in a mesh: ty: 8 (over y, x, core), tx: 4 (over z).
Axes of the slice: x: 2, y: 2, z: 4, core: 2. Of those that a mesh axis runs over, the one named last changes fastest.
Arguments:
- noise: float32 [1024, 1024], P('ty', 'tx'), may hold values from -6 to 6
- root_spectrum: float32 [384, 512], replicated, may hold values from 0.25 to 4
Outputs:
- field: float32 [1024, 1024], P('ty', 'tx')
The draws below stay inside these ranges and needn't reach their ends.
All inputs are finite; a program needn't handle non-finite values.
Results may differ from the reference program's by a relative error of at most 0.0003.
Values sent between devices are 32-bit elements; how exact they have to be, the bound alone decides.
No kernel may reach another device: no remote copies, remote signals or barrier semaphores. Data moves between devices by JAX's collectives and lax.ppermute only.
A program may use at most 64 MiB of HBM per device.

```python
import math
import jax
import jax.numpy as jnp
from jax import lax

MARGIN = 128
CY = 128
CX = 256
EY = 384
EX = 512
NY = 1024
NX = 1024
N_TY = 8
N_TX = 4


def block_levels(own_key, dims, cuts, smallest, top_value):
    def one(dim, shards_of):
        draws = jax.random.uniform(jax.random.fold_in(jax.random.fold_in(own_key, 6), dim), (shards_of,), jnp.float32, smallest / len(cuts), top_value / len(cuts))
        return jnp.repeat(jnp.exp(draws), dims[dim] // shards_of).reshape((-1,) + (1,) * (len(dims) - dim - 1))

    factor_of = one(*cuts[0])
    for cut in cuts[1:]:
        factor_of = factor_of * one(*cut)
    return factor_of


def normal_values(stream_key, shape, deviation, reach, split=(), kind=jnp.bfloat16):
    level = block_levels(stream_key, shape, split, -0.22, 0.18) if split else 1.0
    values = jax.random.normal(stream_key, shape, jnp.float32) * deviation * level
    return jnp.minimum(jnp.maximum(values, -reach), reach).astype(kind)


def setup_inputs(seed: int = 0) -> dict:
    key_list = jax.random.split(jax.random.key(seed), 3)
    return {
        "noise": normal_values(key_list[0], (NY, NX), 1.0, 6.0, ((0, 8), (1, 4)), jnp.float32),
        "root_spectrum": jnp.clip(jnp.exp(jax.random.uniform(key_list[1], (EY, EX), jnp.float32, math.log(0.25), math.log(4.0))), 0.25, 4.0),
    }


def blend_weights(margin, rows_total, cols_total):
    knots = (jnp.arange(rows_total, dtype=jnp.float32) + 0.5) / margin
    weight_rows = jnp.where(knots < 1.0, 0.5 * knots * knots,
                            jnp.where(knots < 2.0, 0.5 * (-2.0 * knots * knots + 6.0 * knots - 3.0),
                                      0.5 * (3.0 - knots) * (3.0 - knots)))
    columns = jnp.arange(cols_total, dtype=jnp.float32) + 0.5
    weight_cols = 1.0 - jnp.abs(columns - 2.0 * margin) / (2.0 * margin)
    return weight_rows[:, None] * weight_cols[None, :]


def reference(noise, root_spectrum):
    margin = MARGIN
    padded = jnp.pad(noise, ((margin, margin), (margin, margin)), mode="wrap")
    weights = blend_weights(margin, EY, EX)

    def place(total, counter):
        row_tile = (counter // N_TX).astype(jnp.int32)
        col_tile = (counter % N_TX).astype(jnp.int32)
        start_row = (row_tile * CY).astype(jnp.int32)
        start_col = (col_tile * CX).astype(jnp.int32)
        window = lax.dynamic_slice(padded, (start_row, start_col), (EY, EX))
        sample = jnp.real(jnp.fft.ifft2(root_spectrum * jnp.fft.fft2(window)))
        blended = sample * weights
        current = lax.dynamic_slice(total, (start_row, start_col), (EY, EX))
        total = lax.dynamic_update_slice(total, current + blended, (start_row, start_col))
        return total, None

    start = jnp.zeros(padded.shape, padded.dtype)
    total, _ = lax.scan(place, start, jnp.arange(N_TY * N_TX, dtype=jnp.int32))
    folded = total[margin:margin + NY]
    folded = folded.at[NY - margin:].add(total[:margin])
    folded = folded.at[:margin].add(total[margin + NY:])
    result = folded[:, margin:margin + NX]
    result = result.at[:, NX - margin:].add(folded[:, :margin])
    result = result.at[:, :margin].add(folded[:, margin + NX:])
    return result
```

```python
import functools
import math

import numpy as np
import jax
import jax.numpy as jnp
from jax import lax
from jax.experimental import pallas as pl
from jax.experimental.pallas import tpu as pltpu
from jax.sharding import PartitionSpec as P

F32 = jnp.float32
BF16 = jnp.bfloat16


def halves(table):
    high = table.astype(BF16)
    low = (table - high.astype(np.float64)).astype(BF16)
    return [high, low]


def row_tables(cols):
    half = cols // 2
    quarter = cols // 4
    c = np.arange(half)[:, None]
    m = np.arange(quarter)[None, :]
    sign = (1.0 - 2.0 * (np.arange(half) % 2))
    even = 2.0 * np.pi * ((2 * m * c) % cols) / cols
    odd = 2.0 * np.pi * (((2 * m + 1) * c) % cols) / cols
    even_sine = -np.sin(even)
    even_sine[:, 0] = sign
    forward_even = np.concatenate([np.cos(even), even_sine], axis=1)
    forward_odd = np.concatenate([np.cos(odd), -np.sin(odd)], axis=1)
    twice = np.full((half, 1), 2.0)
    twice[0] = 1.0
    twice[quarter] = 1.0
    back_even = forward_even.T * twice
    back_odd = forward_odd.T * 2.0
    return np.stack(halves(forward_even) + halves(forward_odd) + halves(back_even) + halves(back_odd))


def column_tables(rows):
    third = rows // 3
    q = np.arange(third)[:, None]
    s = np.arange(third)[None, :]
    forward = []
    back = []
    for p in range(3):
        angle = 2.0 * np.pi * (((3 * q + p) * s) % rows) / rows
        table = np.block([[np.cos(angle), np.sin(angle)], [-np.sin(angle), np.cos(angle)]])
        forward += halves(table)
        back += halves(table.T)
    return np.stack(forward), np.stack(back)


def mirror_tables(rows):
    third = rows // 3
    eye = np.eye(third)
    zero = np.zeros((third, third))
    same = eye[(-np.arange(third)) % third]
    swapped = eye[::-1]
    return np.stack([np.block([[m, zero], [zero, -m]]) for m in (same, swapped)]).astype(BF16)


def split(values):
    high = values.astype(BF16)
    return high, (values - high.astype(F32)).astype(BF16)


def dot(left, right):
    return jnp.dot(left, right, preferred_element_type=F32)


def by_table(values, high, low):
    first, second = split(values)
    return dot(first, high) + dot(second, high) + dot(first, low)


def from_table(high, low, values):
    first, second = split(values)
    return dot(high, first) + dot(high, second) + dot(low, first)


def spectrum_kernel(root_ref, mixed_ref, crossed_ref):
    rows, cols = root_ref.shape
    third = rows // 3
    half = cols // 2
    quarter = cols // 4
    root = root_ref[...]
    k = lax.broadcasted_iota(jnp.int32, (cols, half), 0)
    lane = lax.broadcasted_iota(jnp.int32, (cols, half), 1)
    wanted = jnp.where(lane < quarter, 2 * lane, 2 * (lane - quarter) + 1)
    mirrored = jnp.where(wanted == 0, 0, cols - wanted)
    first_lane = lane == 0
    share = jnp.where(first_lane, 0.5, 1.0)
    nyquist = jnp.logical_and(first_lane, k == half)
    pick = jnp.where(jnp.logical_or(k == wanted, nyquist), share, 0.0).astype(BF16)
    pick_mirrored = jnp.where(jnp.logical_or(k == mirrored, nyquist), share, 0.0).astype(BF16)
    high, low = split(root)
    chosen = dot(high, pick) + dot(low, pick)
    chosen_mirrored = dot(high, pick_mirrored) + dot(low, pick_mirrored)
    difference = 0.5 * (root[:, :quarter] - root[:, half:half + quarter])
    i = lax.broadcasted_iota(jnp.int32, (third, rows), 0)
    j = lax.broadcasted_iota(jnp.int32, (third, rows), 1)
    scale = 0.5 / (rows * cols)
    c_high, c_low = split(chosen)
    m_high, m_low = split(chosen_mirrored)
    d_high, d_low = split(difference)
    block_lane = lax.broadcasted_iota(jnp.int32, (third, quarter), 1)
    for p in range(3):
        source = 3 * i + p
        target = rows - source
        target = jnp.where(target == rows, 0, target)
        order = jnp.where(j == source, 1.0, 0.0).astype(BF16)
        order_mirrored = jnp.where(j == target, 1.0, 0.0).astype(BF16)
        both = jnp.where(j == source, 1.0, 0.0) + jnp.where(j == target, 1.0, 0.0)
        both = both.astype(BF16)
        mixed = dot(order, c_high) + dot(order, c_low) + dot(order_mirrored, m_high) + dot(order_mirrored, m_low)
        mixed_ref[p * third:(p + 1) * third, :] = mixed * scale
        crossed = dot(both, d_high) + dot(both, d_low)
        crossed_ref[p * third:(p + 1) * third, :] = jnp.where(block_lane == 0, crossed * scale, 0.0)


def filter_kernel(mid_0, mid_1, mid_2, side_0, side_1, side_2, mixed_ref, crossed_ref, row_ref, forward_ref, back_ref,
                  mirror_ref, mid_out_0, mid_out_1, mid_out_2, side_out_0, side_out_1, side_out_2, real_ref, imag_ref,
                  spec_ref):
    third = mid_0.shape[0]
    half = mid_0.shape[1]
    quarter = half // 2
    root_three = math.sqrt(3.0) / 2.0
    for j, (mid, side) in enumerate(((mid_0, side_0), (mid_1, side_1), (mid_2, side_2))):
        left = side[:, :quarter]
        right = side[:, quarter:]
        first = mid[:, :quarter]
        second = mid[:, quarter:]
        even = jnp.concatenate([left + second, first + right], axis=1)
        odd = jnp.concatenate([left - second, first - right], axis=1)
        even = by_table(even, row_ref[0], row_ref[1])
        odd = by_table(odd, row_ref[2], row_ref[3])
        real_ref[j, :, :quarter] = even[:, :quarter]
        real_ref[j, :, quarter:] = odd[:, :quarter]
        imag_ref[j, :, :quarter] = even[:, quarter:]
        imag_ref[j, :, quarter:] = odd[:, quarter:]
    sum_real = real_ref[1] + real_ref[2]
    sum_imag = imag_ref[1] + imag_ref[2]
    gap_real = root_three * (real_ref[1] - real_ref[2])
    gap_imag = root_three * (imag_ref[1] - imag_ref[2])
    base_real = real_ref[0] - 0.5 * sum_real
    base_imag = imag_ref[0] - 0.5 * sum_imag
    inputs = (
        (real_ref[0] + sum_real, imag_ref[0] + sum_imag),
        (base_real + gap_imag, base_imag - gap_real),
        (base_real - gap_imag, base_imag + gap_real),
    )
    for p, pair in enumerate(inputs):
        stacked = jnp.concatenate(pair, axis=0)
        spec_ref[p] = from_table(forward_ref[2 * p], forward_ref[2 * p + 1], stacked)
    packed = []
    for p in range(3):
        high, low = split(spec_ref[(3 - p) % 3, :, :quarter])
        flipped = dot(mirror_ref[min(p, 1)], jnp.concatenate([high, low], axis=1))
        packed.append(flipped[:, :quarter] + flipped[:, quarter:])
    outs = []
    for p in range(3):
        mixed = mixed_ref[p * third:(p + 1) * third, :]
        mixed = jnp.concatenate([mixed, mixed], axis=0)
        crossed = crossed_ref[p * third:(p + 1) * third, :]
        crossed = jnp.concatenate([crossed, crossed], axis=0)
        filtered = spec_ref[p] * mixed
        filtered = jnp.concatenate([filtered[:, :quarter] + packed[p] * crossed, filtered[:, quarter:]], axis=1)
        outs.append(from_table(back_ref[2 * p], back_ref[2 * p + 1], filtered))
    real = [value[:third] for value in outs]
    imag = [value[third:] for value in outs]
    sum_real = real[1] + real[2]
    sum_imag = imag[1] + imag[2]
    gap_real = root_three * (real[1] - real[2])
    gap_imag = root_three * (imag[1] - imag[2])
    base_real = real[0] - 0.5 * sum_real
    base_imag = imag[0] - 0.5 * sum_imag
    blocks = (
        (real[0] + sum_real, imag[0] + sum_imag),
        (base_real - gap_imag, base_imag + gap_real),
        (base_real + gap_imag, base_imag - gap_real),
    )
    lane = lax.broadcasted_iota(jnp.int32, (1, half), 1).astype(F32)
    rising = (lane + 0.5) / half
    falling = 1.0 - rising
    row = lax.broadcasted_iota(jnp.int32, (third, 1), 0).astype(F32)
    for j, (block, mid_out, side_out) in enumerate(
        zip(blocks, (mid_out_0, mid_out_1, mid_out_2), (side_out_0, side_out_1, side_out_2))
    ):
        knots = (row + 0.5) / third + j
        if j == 0:
            weight = 0.5 * knots * knots
        elif j == 1:
            weight = 0.5 * (-2.0 * knots * knots + 6.0 * knots - 3.0)
        else:
            weight = 0.5 * (3.0 - knots) * (3.0 - knots)
        even = jnp.concatenate([block[0][:, :quarter], block[1][:, :quarter]], axis=1)
        odd = jnp.concatenate([block[0][:, quarter:], block[1][:, quarter:]], axis=1)
        even = by_table(even, row_ref[4], row_ref[5])
        odd = by_table(odd, row_ref[6], row_ref[7])
        lower = (even + odd) * (weight * rising)
        upper = (even - odd) * (weight * falling)
        side_out[:, :quarter] = lower[:, :quarter]
        side_out[:, quarter:] = upper[:, quarter:]
        mid_out[:, :quarter] = lower[:, quarter:]
        mid_out[:, quarter:] = upper[:, :quarter]


def whole(count):
    return [pl.BlockSpec(memory_space=pltpu.VMEM)] * count


def passed_along(shard, axis, by):
    length = lax.axis_size(axis)
    return lax.ppermute(shard, axis, [(i, (i + by) % length) for i in range(length)])


def per_device(noise, root_spectrum):
    margin, block_cols = noise.shape
    rows, cols = root_spectrum.shape
    row_table = jnp.asarray(row_tables(cols))
    forward_table, back_table = (jnp.asarray(t) for t in column_tables(rows))
    mirror_table = jnp.asarray(mirror_tables(rows))
    limit = pltpu.CompilerParams(vmem_limit_bytes=24 * 1024 * 1024)
    mixed, crossed = pl.pallas_call(
        spectrum_kernel,
        out_shape=(jax.ShapeDtypeStruct((rows, cols // 2), F32), jax.ShapeDtypeStruct((rows, cols // 4), F32)),
        in_specs=whole(1),
        out_specs=tuple(whole(2)),
        compiler_params=limit,
        cost_estimate=pl.CostEstimate(flops=2 * 10**9, bytes_accessed=10**6, transcendentals=0),
        name="spectrum",
    )(root_spectrum)
    from_left = passed_along(noise[:, block_cols - margin:], "tx", 1)
    from_right = passed_along(noise[:, :margin], "tx", -1)
    upper = passed_along(noise, "ty", 1)
    lower = passed_along(noise, "ty", -1)
    side = jnp.concatenate([from_left, from_right], axis=1)
    upper_side = passed_along(side, "ty", 1)
    lower_side = passed_along(side, "ty", -1)
    block = jax.ShapeDtypeStruct((margin, block_cols), F32)
    mid_0, mid_1, mid_2, side_0, side_1, side_2 = pl.pallas_call(
        filter_kernel,
        out_shape=(block,) * 6,
        in_specs=whole(12),
        out_specs=tuple(whole(6)),
        scratch_shapes=[
            pltpu.VMEM((3, margin, block_cols), F32),
            pltpu.VMEM((3, margin, block_cols), F32),
            pltpu.VMEM((3, 2 * margin, block_cols), F32),
        ],
        compiler_params=limit,
        cost_estimate=pl.CostEstimate(flops=4 * 10**9, bytes_accessed=10**7, transcendentals=0),
        name="filter",
    )(upper, noise, lower, upper_side, side, lower_side, mixed, crossed, row_table, forward_table, back_table,
      mirror_table)
    side = side_1 + passed_along(side_0, "ty", -1) + passed_along(side_2, "ty", 1)
    to_right = passed_along(side[:, margin:], "tx", 1)
    to_left = passed_along(side[:, :margin], "tx", -1)
    mid = mid_1 + passed_along(mid_0, "ty", -1) + passed_along(mid_2, "ty", 1)
    return mid + jnp.concatenate([to_right, to_left], axis=1)


def solution(mesh):
    placed = (P("ty", "tx"), P())
    return jax.shard_map(
        per_device, mesh=mesh, in_specs=placed, out_specs=P("ty", "tx"), check_vma=False
    )
```

```python
import math

import numpy as np
import jax
import jax.numpy as jnp
from jax import lax
from jax.experimental import pallas as pl
from jax.experimental.pallas import tpu as pltpu
from jax.sharding import PartitionSpec as P


F32 = jnp.float32
BF16 = jnp.bfloat16


def halves(table):
    high = table.astype(BF16)
    low = (table - high.astype(np.float64)).astype(BF16)
    return [high, low]


def row_tables(cols):
    half = cols // 2
    quarter = cols // 4
    c = np.arange(half)[:, None]
    m = np.arange(quarter)[None, :]
    sign = (1.0 - 2.0 * (np.arange(half) % 2))
    even = 2.0 * np.pi * ((2 * m * c) % cols) / cols
    odd = 2.0 * np.pi * (((2 * m + 1) * c) % cols) / cols
    even_sine = -np.sin(even)
    even_sine[:, 0] = sign
    forward_even = np.concatenate([np.cos(even), even_sine], axis=1)
    forward_odd = np.concatenate([np.cos(odd), -np.sin(odd)], axis=1)
    twice = np.full((half, 1), 2.0)
    twice[0] = 1.0
    twice[quarter] = 1.0
    back_even = forward_even.T * twice
    back_odd = forward_odd.T * 2.0
    return np.stack(halves(forward_even) + halves(forward_odd) + halves(back_even) + halves(back_odd))


def column_tables(rows):
    third = rows // 3
    q = np.arange(third)[:, None]
    s = np.arange(third)[None, :]
    forward = []
    back = []
    for p in range(3):
        angle = 2.0 * np.pi * (((3 * q + p) * s) % rows) / rows
        table = np.block([[np.cos(angle), np.sin(angle)], [-np.sin(angle), np.cos(angle)]])
        forward += halves(table)
        back += halves(table.T)
    return np.stack(forward), np.stack(back)


def mirror_tables(rows):
    third = rows // 3
    eye = np.eye(third)
    zero = np.zeros((third, third))
    same = eye[(-np.arange(third)) % third]
    swapped = eye[::-1]
    return np.stack([np.block([[m, zero], [zero, -m]]) for m in (same, swapped)]).astype(BF16)


def split(values):
    high = values.astype(BF16)
    return high, (values - high.astype(F32)).astype(BF16)


def dot(left, right):
    return jnp.dot(left, right, preferred_element_type=F32)


def by_table(values, high, low):
    first, second = split(values)
    return dot(first, high) + dot(second, high) + dot(first, low)


def from_table(high, low, values):
    first, second = split(values)
    return dot(high, first) + dot(high, second) + dot(low, first)


def spectrum_kernel(root_ref, mixed_ref, crossed_ref):
    rows, cols = root_ref.shape
    third = rows // 3
    half = cols // 2
    quarter = cols // 4
    root = root_ref[...]
    k = lax.broadcasted_iota(jnp.int32, (cols, half), 0)
    lane = lax.broadcasted_iota(jnp.int32, (cols, half), 1)
    wanted = jnp.where(lane < quarter, 2 * lane, 2 * (lane - quarter) + 1)
    mirrored = jnp.where(wanted == 0, 0, cols - wanted)
    first_lane = lane == 0
    share = jnp.where(first_lane, 0.5, 1.0)
    nyquist = jnp.logical_and(first_lane, k == half)
    pick = jnp.where(jnp.logical_or(k == wanted, nyquist), share, 0.0).astype(BF16)
    pick_mirrored = jnp.where(jnp.logical_or(k == mirrored, nyquist), share, 0.0).astype(BF16)
    high, low = split(root)
    chosen = dot(high, pick) + dot(low, pick)
    chosen_mirrored = dot(high, pick_mirrored) + dot(low, pick_mirrored)
    difference = 0.5 * (root[:, :quarter] - root[:, half:half + quarter])
    i = lax.broadcasted_iota(jnp.int32, (third, rows), 0)
    j = lax.broadcasted_iota(jnp.int32, (third, rows), 1)
    scale = 0.5 / (rows * cols)
    c_high, c_low = split(chosen)
    m_high, m_low = split(chosen_mirrored)
    d_high, d_low = split(difference)
    block_lane = lax.broadcasted_iota(jnp.int32, (third, quarter), 1)
    for p in range(3):
        source = 3 * i + p
        target = rows - source
        target = jnp.where(target == rows, 0, target)
        order = jnp.where(j == source, 1.0, 0.0).astype(BF16)
        order_mirrored = jnp.where(j == target, 1.0, 0.0).astype(BF16)
        both = jnp.where(j == source, 1.0, 0.0) + jnp.where(j == target, 1.0, 0.0)
        both = both.astype(BF16)
        mixed = dot(order, c_high) + dot(order, c_low) + dot(order_mirrored, m_high) + dot(order_mirrored, m_low)
        mixed_ref[p * third:(p + 1) * third, :] = mixed * scale
        crossed = dot(both, d_high) + dot(both, d_low)
        crossed_ref[p * third:(p + 1) * third, :] = jnp.where(block_lane == 0, crossed * scale, 0.0)


def swapped(odd, first, second):
    return jnp.where(odd, second, first), jnp.where(odd, first, second)


def filter_kernel(mid_far, mid_own, mid_near, far_far, far_own, far_near, near_far, near_own, near_near, mixed_ref,
                  crossed_ref, row_ref, forward_ref, back_ref, mirror_ref, mid_far_out, mid_own_out, mid_near_out,
                  far_far_out, far_own_out, far_near_out, near_far_out, near_own_out, near_near_out, real_ref, imag_ref,
                  spec_ref):
    third, half = mid_own.shape
    quarter = half // 2
    root_three = math.sqrt(3.0) / 2.0
    odd_row = lax.axis_index("ty") % 2 == 1
    odd_col = lax.axis_index("tx") % 2 == 1
    mid_0, mid_2 = swapped(odd_row, mid_far[...], mid_near[...])
    far_0, far_2 = swapped(odd_row, far_far[...], far_near[...])
    near_0, near_2 = swapped(odd_row, near_far[...], near_near[...])
    parts = ((mid_0, far_0, near_0), (mid_own[...], far_own[...], near_own[...]), (mid_2, far_2, near_2))
    for j, (mid, far, near) in enumerate(parts):
        left, right = swapped(odd_col, far, near)
        first = mid[:, :quarter]
        second = mid[:, quarter:]
        even = jnp.concatenate([left + second, first + right], axis=1)
        odd = jnp.concatenate([left - second, first - right], axis=1)
        even = by_table(even, row_ref[0], row_ref[1])
        odd = by_table(odd, row_ref[2], row_ref[3])
        real_ref[j, :, :quarter] = even[:, :quarter]
        real_ref[j, :, quarter:] = odd[:, :quarter]
        imag_ref[j, :, :quarter] = even[:, quarter:]
        imag_ref[j, :, quarter:] = odd[:, quarter:]
    sum_real = real_ref[1] + real_ref[2]
    sum_imag = imag_ref[1] + imag_ref[2]
    gap_real = root_three * (real_ref[1] - real_ref[2])
    gap_imag = root_three * (imag_ref[1] - imag_ref[2])
    base_real = real_ref[0] - 0.5 * sum_real
    base_imag = imag_ref[0] - 0.5 * sum_imag
    inputs = (
        (real_ref[0] + sum_real, imag_ref[0] + sum_imag),
        (base_real + gap_imag, base_imag - gap_real),
        (base_real - gap_imag, base_imag + gap_real),
    )
    for p, pair in enumerate(inputs):
        stacked = jnp.concatenate(pair, axis=0)
        spec_ref[p] = from_table(forward_ref[2 * p], forward_ref[2 * p + 1], stacked)
    packed = []
    for p in range(3):
        high, low = split(spec_ref[(3 - p) % 3, :, :quarter])
        flipped = dot(mirror_ref[min(p, 1)], jnp.concatenate([high, low], axis=1))
        packed.append(flipped[:, :quarter] + flipped[:, quarter:])
    outs = []
    for p in range(3):
        mixed = mixed_ref[p * third:(p + 1) * third, :]
        mixed = jnp.concatenate([mixed, mixed], axis=0)
        crossed = crossed_ref[p * third:(p + 1) * third, :]
        crossed = jnp.concatenate([crossed, crossed], axis=0)
        filtered = spec_ref[p] * mixed
        filtered = jnp.concatenate([filtered[:, :quarter] + packed[p] * crossed, filtered[:, quarter:]], axis=1)
        outs.append(from_table(back_ref[2 * p], back_ref[2 * p + 1], filtered))
    real = [value[:third] for value in outs]
    imag = [value[third:] for value in outs]
    sum_real = real[1] + real[2]
    sum_imag = imag[1] + imag[2]
    gap_real = root_three * (real[1] - real[2])
    gap_imag = root_three * (imag[1] - imag[2])
    base_real = real[0] - 0.5 * sum_real
    base_imag = imag[0] - 0.5 * sum_imag
    blocks = (
        (real[0] + sum_real, imag[0] + sum_imag),
        (base_real - gap_imag, base_imag + gap_real),
        (base_real + gap_imag, base_imag - gap_real),
    )
    lane = lax.broadcasted_iota(jnp.int32, (1, half), 1).astype(F32)
    rising = (lane + 0.5) / half
    falling = 1.0 - rising
    row = lax.broadcasted_iota(jnp.int32, (third, 1), 0).astype(F32)
    mids = []
    fars = []
    nears = []
    for j, block in enumerate(blocks):
        knots = (row + 0.5) / third + j
        if j == 0:
            weight = 0.5 * knots * knots
        elif j == 1:
            weight = 0.5 * (-2.0 * knots * knots + 6.0 * knots - 3.0)
        else:
            weight = 0.5 * (3.0 - knots) * (3.0 - knots)
        even = jnp.concatenate([block[0][:, :quarter], block[1][:, :quarter]], axis=1)
        odd = jnp.concatenate([block[0][:, quarter:], block[1][:, quarter:]], axis=1)
        even = by_table(even, row_ref[4], row_ref[5])
        odd = by_table(odd, row_ref[6], row_ref[7])
        lower = (even + odd) * (weight * rising)
        upper = (even - odd) * (weight * falling)
        far, near = swapped(odd_col, lower[:, :quarter], upper[:, quarter:])
        fars.append(far)
        nears.append(near)
        mids.append(jnp.concatenate([lower[:, quarter:], upper[:, :quarter]], axis=1))
    far_own_out[...] = fars[1]
    near_own_out[...] = nears[1]
    mid_own_out[...] = mids[1]
    far_far_out[...], far_near_out[...] = swapped(odd_row, fars[0], fars[2])
    near_far_out[...], near_near_out[...] = swapped(odd_row, nears[0], nears[2])
    mid_far_out[...], mid_near_out[...] = swapped(odd_row, mids[0], mids[2])


def whole(count):
    return [pl.BlockSpec(memory_space=pltpu.VMEM)] * count


def exchanged(to_far, to_near, axis):
    count = lax.axis_size(axis)
    assert count % 2 == 0
    far = [(i, (i - 1 + 2 * (i % 2)) % count) for i in range(count)]
    near = [(i, (i + 1 - 2 * (i % 2)) % count) for i in range(count)]
    from_far = lax.ppermute(to_far, axis, far)
    from_near = lax.ppermute(to_near, axis, near)
    return from_far, from_near


def per_device(noise, root_spectrum):
    margin, block_cols = noise.shape
    rows, cols = root_spectrum.shape
    row_table = jnp.asarray(row_tables(cols))
    forward_table, back_table = (jnp.asarray(t) for t in column_tables(rows))
    mirror_table = jnp.asarray(mirror_tables(rows))
    limit = pltpu.CompilerParams(vmem_limit_bytes=24 * 1024 * 1024)
    odd_col = lax.axis_index("tx") % 2 == 1
    mixed, crossed = pl.pallas_call(
        spectrum_kernel,
        out_shape=(jax.ShapeDtypeStruct((rows, cols // 2), F32), jax.ShapeDtypeStruct((rows, cols // 4), F32)),
        in_specs=whole(1),
        out_specs=tuple(whole(2)),
        compiler_params=limit,
        cost_estimate=pl.CostEstimate(flops=2 * 10**9, bytes_accessed=10**6, transcendentals=0),
        name="spectrum",
    )(root_spectrum)
    to_far, to_near = swapped(odd_col, noise[:, :margin], noise[:, block_cols - margin:])
    far, near = exchanged(to_far, to_near, "tx")
    mid_far, mid_near = exchanged(noise, noise, "ty")
    near_far, near_near = exchanged(near, near, "ty")
    far_far, far_near = exchanged(far, far, "ty")
    strip = jax.ShapeDtypeStruct((margin, margin), F32)
    block = jax.ShapeDtypeStruct((margin, block_cols), F32)
    mid_far, mid, mid_near, far_far, far, far_near, near_far, near, near_near = pl.pallas_call(
        filter_kernel,
        out_shape=(block,) * 3 + (strip,) * 6,
        in_specs=whole(15),
        out_specs=tuple(whole(9)),
        scratch_shapes=[
            pltpu.VMEM((3, margin, block_cols), F32),
            pltpu.VMEM((3, margin, block_cols), F32),
            pltpu.VMEM((3, 2 * margin, block_cols), F32),
        ],
        compiler_params=limit,
        cost_estimate=pl.CostEstimate(flops=4 * 10**9, bytes_accessed=10**7, transcendentals=0),
        name="filter",
    )(mid_far, noise, mid_near, far_far, far, far_near, near_far, near, near_near, mixed, crossed, row_table,
      forward_table, back_table, mirror_table)
    far_far, far_near = exchanged(far_far, far_near, "ty")
    near_far, near_near = exchanged(near_far, near_near, "ty")
    mid_far, mid_near = exchanged(mid_far, mid_near, "ty")
    from_far, from_near = exchanged(far + far_far + far_near, near + near_far + near_near, "tx")
    mid = mid + mid_far + mid_near
    return mid + jnp.concatenate(swapped(odd_col, from_far, from_near), axis=1)


def solution(mesh):
    placed = (P("ty", "tx"), P())
    return jax.shard_map(per_device, mesh=mesh, in_specs=placed, out_specs=P("ty", "tx"), check_vma=False)
```

```python
import math

import numpy as np
import jax
import jax.numpy as jnp
from jax import lax
from jax.experimental import pallas as pl
from jax.experimental.pallas import tpu as pltpu
from jax.sharding import PartitionSpec as P


F32 = jnp.float32
BF16 = jnp.bfloat16


def halves(table):
    high = table.astype(BF16)
    low = (table - high.astype(np.float64)).astype(BF16)
    return [high, low]


def row_tables(cols):
    half = cols // 2
    quarter = cols // 4
    c = np.arange(half)[:, None]
    m = np.arange(quarter)[None, :]
    sign = (1.0 - 2.0 * (np.arange(half) % 2))
    even = 2.0 * np.pi * ((2 * m * c) % cols) / cols
    odd = 2.0 * np.pi * (((2 * m + 1) * c) % cols) / cols
    even_sine = -np.sin(even)
    even_sine[:, 0] = sign
    forward_even = np.concatenate([np.cos(even), even_sine], axis=1)
    forward_odd = np.concatenate([np.cos(odd), -np.sin(odd)], axis=1)
    twice = np.full((half, 1), 2.0)
    twice[0] = 1.0
    twice[quarter] = 1.0
    back_even = forward_even.T * twice
    back_odd = forward_odd.T * 2.0
    return np.stack(halves(forward_even) + halves(forward_odd) + halves(back_even) + halves(back_odd))


def column_tables(rows):
    third = rows // 3
    q = np.arange(third)[:, None]
    s = np.arange(third)[None, :]
    forward = []
    back = []
    for p in range(3):
        angle = 2.0 * np.pi * (((3 * q + p) * s) % rows) / rows
        table = np.block([[np.cos(angle), np.sin(angle)], [-np.sin(angle), np.cos(angle)]])
        forward += halves(table)
        back += halves(table.T)
    return np.stack(forward), np.stack(back)


def mirror_tables(rows):
    third = rows // 3
    eye = np.eye(third)
    zero = np.zeros((third, third))
    same = eye[(-np.arange(third)) % third]
    swapped = eye[::-1]
    return np.stack([np.block([[m, zero], [zero, -m]]) for m in (same, swapped)]).astype(BF16)


def split(values):
    high = values.astype(BF16)
    return high, (values - high.astype(F32)).astype(BF16)


def dot(left, right):
    return jnp.dot(left, right, preferred_element_type=F32)


def by_table(values, high, low):
    first, second = split(values)
    return dot(first, high) + dot(second, high) + dot(first, low)


def from_table(high, low, values):
    first, second = split(values)
    return dot(high, first) + dot(high, second) + dot(low, first)


def spectrum_kernel(root_ref, mixed_ref, crossed_ref):
    rows, cols = root_ref.shape
    third = rows // 3
    half = cols // 2
    quarter = cols // 4
    root = root_ref[...]
    k = lax.broadcasted_iota(jnp.int32, (cols, half), 0)
    lane = lax.broadcasted_iota(jnp.int32, (cols, half), 1)
    wanted = jnp.where(lane < quarter, 2 * lane, 2 * (lane - quarter) + 1)
    mirrored = jnp.where(wanted == 0, 0, cols - wanted)
    first_lane = lane == 0
    share = jnp.where(first_lane, 0.5, 1.0)
    nyquist = jnp.logical_and(first_lane, k == half)
    pick = jnp.where(jnp.logical_or(k == wanted, nyquist), share, 0.0).astype(BF16)
    pick_mirrored = jnp.where(jnp.logical_or(k == mirrored, nyquist), share, 0.0).astype(BF16)
    high, low = split(root)
    chosen = dot(high, pick) + dot(low, pick)
    chosen_mirrored = dot(high, pick_mirrored) + dot(low, pick_mirrored)
    difference = 0.5 * (root[:, :quarter] - root[:, half:half + quarter])
    i = lax.broadcasted_iota(jnp.int32, (third, rows), 0)
    j = lax.broadcasted_iota(jnp.int32, (third, rows), 1)
    scale = 0.5 / (rows * cols)
    c_high, c_low = split(chosen)
    m_high, m_low = split(chosen_mirrored)
    d_high, d_low = split(difference)
    block_lane = lax.broadcasted_iota(jnp.int32, (third, quarter), 1)
    for p in range(3):
        source = 3 * i + p
        target = rows - source
        target = jnp.where(target == rows, 0, target)
        order = jnp.where(j == source, 1.0, 0.0).astype(BF16)
        order_mirrored = jnp.where(j == target, 1.0, 0.0).astype(BF16)
        both = jnp.where(j == source, 1.0, 0.0) + jnp.where(j == target, 1.0, 0.0)
        both = both.astype(BF16)
        mixed = dot(order, c_high) + dot(order, c_low) + dot(order_mirrored, m_high) + dot(order_mirrored, m_low)
        mixed_ref[p * third:(p + 1) * third, :] = mixed * scale
        crossed = dot(both, d_high) + dot(both, d_low)
        crossed_ref[p * third:(p + 1) * third, :] = jnp.where(block_lane == 0, crossed * scale, 0.0)


def swapped(odd, first, second):
    return jnp.where(odd, second, first), jnp.where(odd, first, second)


def filter_kernel(mid_far, mid_own, mid_near, left_far, left_own, left_near, right_far, right_own, right_near, mixed_ref,
                  crossed_ref, row_ref, forward_ref, back_ref, mirror_ref, mid_far_out, mid_own_out, mid_near_out,
                  left_far_out, left_own_out, left_near_out, right_far_out, right_own_out, right_near_out, real_ref, imag_ref,
                  spec_ref):
    third, half = mid_own.shape
    quarter = half // 2
    root_three = math.sqrt(3.0) / 2.0
    odd_row = lax.axis_index("ty") % 2 == 1
    mid_0, mid_2 = swapped(odd_row, mid_far[...], mid_near[...])
    left_0, left_2 = swapped(odd_row, left_far[...], left_near[...])
    right_0, right_2 = swapped(odd_row, right_far[...], right_near[...])
    parts = ((mid_0, left_0, right_0), (mid_own[...], left_own[...], right_own[...]), (mid_2, left_2, right_2))
    for j, (mid, left, right) in enumerate(parts):
        first = mid[:, :quarter]
        second = mid[:, quarter:]
        even = jnp.concatenate([left + second, first + right], axis=1)
        odd = jnp.concatenate([left - second, first - right], axis=1)
        even = by_table(even, row_ref[0], row_ref[1])
        odd = by_table(odd, row_ref[2], row_ref[3])
        real_ref[j, :, :quarter] = even[:, :quarter]
        real_ref[j, :, quarter:] = odd[:, :quarter]
        imag_ref[j, :, :quarter] = even[:, quarter:]
        imag_ref[j, :, quarter:] = odd[:, quarter:]
    sum_real = real_ref[1] + real_ref[2]
    sum_imag = imag_ref[1] + imag_ref[2]
    gap_real = root_three * (real_ref[1] - real_ref[2])
    gap_imag = root_three * (imag_ref[1] - imag_ref[2])
    base_real = real_ref[0] - 0.5 * sum_real
    base_imag = imag_ref[0] - 0.5 * sum_imag
    inputs = (
        (real_ref[0] + sum_real, imag_ref[0] + sum_imag),
        (base_real + gap_imag, base_imag - gap_real),
        (base_real - gap_imag, base_imag + gap_real),
    )
    for p, pair in enumerate(inputs):
        stacked = jnp.concatenate(pair, axis=0)
        spec_ref[p] = from_table(forward_ref[2 * p], forward_ref[2 * p + 1], stacked)
    packed = []
    for p in range(3):
        high, low = split(spec_ref[(3 - p) % 3, :, :quarter])
        flipped = dot(mirror_ref[min(p, 1)], jnp.concatenate([high, low], axis=1))
        packed.append(flipped[:, :quarter] + flipped[:, quarter:])
    outs = []
    for p in range(3):
        mixed = mixed_ref[p * third:(p + 1) * third, :]
        mixed = jnp.concatenate([mixed, mixed], axis=0)
        crossed = crossed_ref[p * third:(p + 1) * third, :]
        crossed = jnp.concatenate([crossed, crossed], axis=0)
        filtered = spec_ref[p] * mixed
        filtered = jnp.concatenate([filtered[:, :quarter] + packed[p] * crossed, filtered[:, quarter:]], axis=1)
        outs.append(from_table(back_ref[2 * p], back_ref[2 * p + 1], filtered))
    real = [value[:third] for value in outs]
    imag = [value[third:] for value in outs]
    sum_real = real[1] + real[2]
    sum_imag = imag[1] + imag[2]
    gap_real = root_three * (real[1] - real[2])
    gap_imag = root_three * (imag[1] - imag[2])
    base_real = real[0] - 0.5 * sum_real
    base_imag = imag[0] - 0.5 * sum_imag
    blocks = (
        (real[0] + sum_real, imag[0] + sum_imag),
        (base_real - gap_imag, base_imag + gap_real),
        (base_real + gap_imag, base_imag - gap_real),
    )
    lane = lax.broadcasted_iota(jnp.int32, (1, half), 1).astype(F32)
    rising = (lane + 0.5) / half
    falling = 1.0 - rising
    row = lax.broadcasted_iota(jnp.int32, (third, 1), 0).astype(F32)
    mids = []
    lefts = []
    rights = []
    for j, block in enumerate(blocks):
        knots = (row + 0.5) / third + j
        if j == 0:
            weight = 0.5 * knots * knots
        elif j == 1:
            weight = 0.5 * (-2.0 * knots * knots + 6.0 * knots - 3.0)
        else:
            weight = 0.5 * (3.0 - knots) * (3.0 - knots)
        even = jnp.concatenate([block[0][:, :quarter], block[1][:, :quarter]], axis=1)
        odd = jnp.concatenate([block[0][:, quarter:], block[1][:, quarter:]], axis=1)
        even = by_table(even, row_ref[4], row_ref[5])
        odd = by_table(odd, row_ref[6], row_ref[7])
        lower = (even + odd) * (weight * rising)
        upper = (even - odd) * (weight * falling)
        lefts.append(lower[:, :quarter])
        rights.append(upper[:, quarter:])
        mids.append(jnp.concatenate([lower[:, quarter:], upper[:, :quarter]], axis=1))
    left_own_out[...] = lefts[1]
    right_own_out[...] = rights[1]
    mid_own_out[...] = mids[1]
    left_far_out[...], left_near_out[...] = swapped(odd_row, lefts[0], lefts[2])
    right_far_out[...], right_near_out[...] = swapped(odd_row, rights[0], rights[2])
    mid_far_out[...], mid_near_out[...] = swapped(odd_row, mids[0], mids[2])


def whole(count):
    return [pl.BlockSpec(memory_space=pltpu.VMEM)] * count


def passed_along(shard, axis, by):
    count = lax.axis_size(axis)
    return lax.ppermute(shard, axis, [(i, (i + by) % count) for i in range(count)])


def exchanged(to_far, to_near, axis):
    count = lax.axis_size(axis)
    assert count % 2 == 0
    far = [(i, (i - 1 + 2 * (i % 2)) % count) for i in range(count)]
    near = [(i, (i + 1 - 2 * (i % 2)) % count) for i in range(count)]
    from_far = lax.ppermute(to_far, axis, far)
    from_near = lax.ppermute(to_near, axis, near)
    return from_far, from_near


def per_device(noise, root_spectrum):
    margin, block_cols = noise.shape
    rows, cols = root_spectrum.shape
    row_table = jnp.asarray(row_tables(cols))
    forward_table, back_table = (jnp.asarray(t) for t in column_tables(rows))
    mirror_table = jnp.asarray(mirror_tables(rows))
    limit = pltpu.CompilerParams(vmem_limit_bytes=24 * 1024 * 1024)
    mixed, crossed = pl.pallas_call(
        spectrum_kernel,
        out_shape=(jax.ShapeDtypeStruct((rows, cols // 2), F32), jax.ShapeDtypeStruct((rows, cols // 4), F32)),
        in_specs=whole(1),
        out_specs=tuple(whole(2)),
        compiler_params=limit,
        cost_estimate=pl.CostEstimate(flops=2 * 10**9, bytes_accessed=10**6, transcendentals=0),
        name="spectrum",
    )(root_spectrum)
    left = passed_along(noise[:, block_cols - margin:], "tx", 1)
    right = passed_along(noise[:, :margin], "tx", -1)
    mid_far, mid_near = exchanged(noise, noise, "ty")
    left_far, left_near = exchanged(left, left, "ty")
    right_far, right_near = exchanged(right, right, "ty")
    strip = jax.ShapeDtypeStruct((margin, margin), F32)
    block = jax.ShapeDtypeStruct((margin, block_cols), F32)
    mid_far, mid, mid_near, left_far, left_own, left_near, right_far, right, right_near = pl.pallas_call(
        filter_kernel,
        out_shape=(block,) * 3 + (strip,) * 6,
        in_specs=whole(15),
        out_specs=tuple(whole(9)),
        scratch_shapes=[
            pltpu.VMEM((3, margin, block_cols), F32),
            pltpu.VMEM((3, margin, block_cols), F32),
            pltpu.VMEM((3, 2 * margin, block_cols), F32),
        ],
        compiler_params=limit,
        cost_estimate=pl.CostEstimate(flops=4 * 10**9, bytes_accessed=10**7, transcendentals=0),
        name="filter",
    )(mid_far, noise, mid_near, left_far, left, left_near, right_far, right, right_near, mixed, crossed,
      row_table, forward_table, back_table, mirror_table)
    right_far, right_near = exchanged(right_far, right_near, "ty")
    left_far, left_near = exchanged(left_far, left_near, "ty")
    mid_far, mid_near = exchanged(mid_far, mid_near, "ty")
    left = passed_along(right + right_far + right_near, "tx", 1)
    right = passed_along(left_own + left_far + left_near, "tx", -1)
    mid = mid + mid_far + mid_near
    return mid + jnp.concatenate([left, right], axis=1)


def solution(mesh):
    placed = (P("ty", "tx"), P())
    return jax.shard_map(per_device, mesh=mesh, in_specs=placed, out_specs=P("ty", "tx"), check_vma=False)
```

```python
import math

import numpy as np
import jax
import jax.numpy as jnp
from jax import lax
from jax.experimental import pallas as pl
from jax.experimental.pallas import tpu as pltpu
from jax.sharding import PartitionSpec as P


F32 = jnp.float32
BF16 = jnp.bfloat16


def halves(table):
    high = table.astype(BF16)
    low = (table - high.astype(np.float64)).astype(BF16)
    return [high, low]


def row_tables(cols):
    half = cols // 2
    quarter = cols // 4
    c = np.arange(half)[:, None]
    m = np.arange(quarter)[None, :]
    sign = (1.0 - 2.0 * (np.arange(half) % 2))
    even = 2.0 * np.pi * ((2 * m * c) % cols) / cols
    odd = 2.0 * np.pi * (((2 * m + 1) * c) % cols) / cols
    even_sine = -np.sin(even)
    even_sine[:, 0] = sign
    forward_even = np.concatenate([np.cos(even), even_sine], axis=1)
    forward_odd = np.concatenate([np.cos(odd), -np.sin(odd)], axis=1)
    twice = np.full((half, 1), 2.0)
    twice[0] = 1.0
    twice[quarter] = 1.0
    back_even = forward_even.T * twice
    back_odd = forward_odd.T * 2.0
    return np.stack(halves(forward_even) + halves(forward_odd) + halves(back_even) + halves(back_odd))


def column_tables(rows):
    third = rows // 3
    q = np.arange(third)[:, None]
    s = np.arange(third)[None, :]
    forward = []
    back = []
    for p in range(3):
        angle = 2.0 * np.pi * (((3 * q + p) * s) % rows) / rows
        table = np.block([[np.cos(angle), np.sin(angle)], [-np.sin(angle), np.cos(angle)]])
        forward += halves(table)
        back += halves(table.T)
    return np.stack(forward), np.stack(back)


def mirror_tables(rows):
    third = rows // 3
    eye = np.eye(third)
    zero = np.zeros((third, third))
    same = eye[(-np.arange(third)) % third]
    swapped = eye[::-1]
    return np.stack([np.block([[m, zero], [zero, -m]]) for m in (same, swapped)]).astype(BF16)


def split(values):
    high = values.astype(BF16)
    return high, (values - high.astype(F32)).astype(BF16)


def dot(left, right):
    return jnp.dot(left, right, preferred_element_type=F32)


def by_table(values, high, low):
    first, second = split(values)
    return dot(first, high) + dot(second, high) + dot(first, low)


def spectrum_kernel(root_ref, mixed_ref, crossed_ref):
    rows, cols = root_ref.shape
    third = rows // 3
    half = cols // 2
    quarter = cols // 4
    root = root_ref[...]
    k = lax.broadcasted_iota(jnp.int32, (cols, half), 0)
    lane = lax.broadcasted_iota(jnp.int32, (cols, half), 1)
    wanted = jnp.where(lane < quarter, 2 * lane, 2 * (lane - quarter) + 1)
    mirrored = jnp.where(wanted == 0, 0, cols - wanted)
    first_lane = lane == 0
    share = jnp.where(first_lane, 0.5, 1.0)
    nyquist = jnp.logical_and(first_lane, k == half)
    pick = jnp.where(jnp.logical_or(k == wanted, nyquist), share, 0.0).astype(BF16)
    pick_mirrored = jnp.where(jnp.logical_or(k == mirrored, nyquist), share, 0.0).astype(BF16)
    high, low = split(root)
    chosen = dot(high, pick) + dot(low, pick)
    chosen_mirrored = dot(high, pick_mirrored) + dot(low, pick_mirrored)
    difference = 0.5 * (root[:, :quarter] - root[:, half:half + quarter])
    i = lax.broadcasted_iota(jnp.int32, (third, rows), 0)
    j = lax.broadcasted_iota(jnp.int32, (third, rows), 1)
    scale = 0.5 / (rows * cols)
    c_high, c_low = split(chosen)
    m_high, m_low = split(chosen_mirrored)
    d_high, d_low = split(difference)
    block_lane = lax.broadcasted_iota(jnp.int32, (third, quarter), 1)
    for p in range(3):
        source = 3 * i + p
        target = rows - source
        target = jnp.where(target == rows, 0, target)
        order = jnp.where(j == source, 1.0, 0.0).astype(BF16)
        order_mirrored = jnp.where(j == target, 1.0, 0.0).astype(BF16)
        both = jnp.where(j == source, 1.0, 0.0) + jnp.where(j == target, 1.0, 0.0)
        both = both.astype(BF16)
        mixed = dot(order, c_high) + dot(order, c_low) + dot(order_mirrored, m_high) + dot(order_mirrored, m_low)
        mixed_ref[p * third:(p + 1) * third, :] = mixed * scale
        crossed = dot(both, d_high) + dot(both, d_low)
        crossed_ref[p * third:(p + 1) * third, :] = jnp.where(block_lane == 0, crossed * scale, 0.0)


def twice(block):
    return jnp.concatenate([block, block], axis=0)


def thirds(block):
    third = block.shape[0] // 3
    quarter = block.shape[1] // 2
    return [
        (block[j * third:(j + 1) * third, :quarter], block[j * third:(j + 1) * third, quarter:]) for j in range(3)
    ]


def spread(block):
    (real_0, imag_0), (real_1, imag_1), (real_2, imag_2) = thirds(block)
    root_three = math.sqrt(3.0) / 2.0
    sum_real = real_1 + real_2
    sum_imag = imag_1 + imag_2
    gap_real = root_three * (real_1 - real_2)
    gap_imag = root_three * (imag_1 - imag_2)
    base_real = real_0 - 0.5 * sum_real
    base_imag = imag_0 - 0.5 * sum_imag
    return [
        jnp.concatenate([real_0 + sum_real, imag_0 + sum_imag], axis=0),
        jnp.concatenate([base_real + gap_imag, base_imag - gap_real], axis=0),
        jnp.concatenate([base_real - gap_imag, base_imag + gap_real], axis=0),
    ]


def gathered(classes):
    third = classes[0].shape[0] // 2
    real = [value[:third] for value in classes]
    imag = [value[third:] for value in classes]
    root_three = math.sqrt(3.0) / 2.0
    sum_real = real[1] + real[2]
    sum_imag = imag[1] + imag[2]
    gap_real = root_three * (real[1] - real[2])
    gap_imag = root_three * (imag[1] - imag[2])
    base_real = real[0] - 0.5 * sum_real
    base_imag = imag[0] - 0.5 * sum_imag
    blocks = (
        (real[0] + sum_real, imag[0] + sum_imag),
        (base_real - gap_imag, base_imag + gap_real),
        (base_real + gap_imag, base_imag - gap_real),
    )
    return jnp.concatenate([jnp.concatenate(block, axis=1) for block in blocks], axis=0)


def swapped(odd, first, second):
    return jnp.where(odd, second, first), jnp.where(odd, first, second)


def rows_kernel(mid_far, mid_own, mid_near, left_far, left_own, left_near, right_own, tables_ref, even_ref, odd_ref):
    quarter = mid_own.shape[1] // 2
    row_ref = tables_ref.at[:8]
    odd_row = lax.axis_index("ty") % 2 == 1
    mid_0, mid_2 = swapped(odd_row, mid_far[...], mid_near[...])
    left_0, left_2 = swapped(odd_row, left_far[...], left_near[...])
    evens = []
    odds = []
    for mid, left, right in ((mid_0, left_0, None), (mid_own[...], left_own[...], right_own[...]), (mid_2, left_2, None)):
        first = mid[:, :quarter]
        second = mid[:, quarter:]
        plus, minus = (first, first) if right is None else (first + right, first - right)
        evens.append(jnp.concatenate([left + second, plus], axis=1))
        odds.append(jnp.concatenate([left - second, minus], axis=1))
    even_ref[...] = by_table(jnp.concatenate(evens, axis=0), row_ref[0], row_ref[1])
    odd_ref[...] = by_table(jnp.concatenate(odds, axis=0), row_ref[2], row_ref[3])


def added(block, strips, high, low):
    third = block.shape[0] // 3
    quarter = strips[0].shape[1]
    high = high[quarter:]
    share = dot(jnp.concatenate(strips, axis=1), jnp.concatenate([high, high], axis=0)) + dot(strips[0], low[quarter:])
    return jnp.concatenate([block[:third] + share[:third], block[third:2 * third], block[2 * third:] + share[third:]], axis=0)


def filter_kernel(even_ref, odd_ref, right_far, right_near, mixed_ref, crossed_ref, tables_ref, mid_far_out, mid_own_out, mid_near_out, left_far_out, left_own_out, left_near_out,
                  right_far_out, right_own_out, right_near_out):
    third, half = mid_own_out.shape
    row_ref, forward_ref, back_ref, mirror_ref = (tables_ref.at[a:b] for a, b in ((0, 8), (8, 14), (14, 20), (20, 22)))
    quarter = half // 2
    odd_row = lax.axis_index("ty") % 2 == 1
    right = jnp.concatenate(swapped(odd_row, right_far[...], right_near[...]), axis=0)
    even = added(even_ref[...], split(right), row_ref[0], row_ref[1])
    odd = added(odd_ref[...], split(-right), row_ref[2], row_ref[3])
    even_inputs = [split(value) for value in spread(even)]
    even_main = [dot(forward_ref[2 * p], jnp.concatenate(even_inputs[p], axis=1)) for p in range(3)]
    odd_inputs = [split(value) for value in spread(odd)]
    even_spec = []
    odd_spec = []
    for p in range(3):
        odd_main = dot(forward_ref[2 * p], jnp.concatenate(odd_inputs[p], axis=1))
        rest = dot(forward_ref[2 * p + 1], jnp.concatenate([even_inputs[p][0], odd_inputs[p][0]], axis=1))
        even_spec.append(even_main[p][:, :quarter] + even_main[p][:, quarter:] + rest[:, :quarter])
        odd_spec.append(odd_main[:, :quarter] + odd_main[:, quarter:] + rest[:, quarter:])
    even_parts = []
    odd_parts = []
    for p in range(3):
        flipped = dot(mirror_ref[min(p, 1)], jnp.concatenate(split(even_spec[(3 - p) % 3]), axis=1))
        flipped = flipped[:, :quarter] + flipped[:, quarter:]
        rows = slice(p * third, (p + 1) * third)
        even_gain = mixed_ref[rows, :quarter]
        odd_gain = mixed_ref[rows, quarter:]
        crossed = crossed_ref[rows, :]
        filtered = even_spec[p] * twice(even_gain) + flipped * twice(crossed)
        even_parts.append(split(filtered))
        odd_parts.append(split(odd_spec[p] * twice(odd_gain)))
    even_back = []
    rests = []
    for p in range(3):
        main = dot(back_ref[2 * p], jnp.concatenate(even_parts[p], axis=1))
        rest = dot(back_ref[2 * p + 1], jnp.concatenate([even_parts[p][0], odd_parts[p][0]], axis=1))
        even_back.append(main[:, :quarter] + main[:, quarter:] + rest[:, :quarter])
        rests.append(rest[:, quarter:])
    odd_back = []
    for p in range(3):
        main = dot(back_ref[2 * p], jnp.concatenate(odd_parts[p], axis=1))
        odd_back.append(main[:, :quarter] + main[:, quarter:] + rests[p])
    even = by_table(gathered(even_back), row_ref[4], row_ref[5])
    odd = by_table(gathered(odd_back), row_ref[6], row_ref[7])
    lane = lax.broadcasted_iota(jnp.int32, (1, half), 1).astype(F32)
    rising = (lane + 0.5) / half
    falling = 1.0 - rising
    row = lax.broadcasted_iota(jnp.int32, (third, 1), 0).astype(F32)
    mids = []
    lefts = []
    rights = []
    for j in range(3):
        knots = (row + 0.5) / third + j
        if j == 0:
            weight = 0.5 * knots * knots
        elif j == 1:
            weight = 0.5 * (-2.0 * knots * knots + 6.0 * knots - 3.0)
        else:
            weight = 0.5 * (3.0 - knots) * (3.0 - knots)
        rows = slice(j * third, (j + 1) * third)
        lower = (even[rows] + odd[rows]) * (weight * rising)
        upper = (even[rows] - odd[rows]) * (weight * falling)
        lefts.append(lower[:, :quarter])
        rights.append(upper[:, quarter:])
        mids.append(jnp.concatenate([lower[:, quarter:], upper[:, :quarter]], axis=1))
    left_own_out[...] = lefts[1]
    right_own_out[...] = rights[1]
    mid_own_out[...] = mids[1]
    left_far_out[...], left_near_out[...] = swapped(odd_row, lefts[0], lefts[2])
    right_far_out[...], right_near_out[...] = swapped(odd_row, rights[0], rights[2])
    mid_far_out[...], mid_near_out[...] = swapped(odd_row, mids[0], mids[2])


def whole(count):
    return [pl.BlockSpec(memory_space=pltpu.VMEM)] * count


def passed_along(shard, axis, by):
    count = lax.axis_size(axis)
    return lax.ppermute(shard, axis, [(i, (i + by) % count) for i in range(count)])


def exchanged(to_far, to_near, axis):
    count = lax.axis_size(axis)
    assert count % 2 == 0
    far = [(i, (i - 1 + 2 * (i % 2)) % count) for i in range(count)]
    near = [(i, (i + 1 - 2 * (i % 2)) % count) for i in range(count)]
    from_far = lax.ppermute(to_far, axis, far)
    from_near = lax.ppermute(to_near, axis, near)
    return from_far, from_near


def per_device(noise, root_spectrum):
    margin, block_cols = noise.shape
    rows, cols = root_spectrum.shape
    tables = jnp.asarray(np.concatenate([row_tables(cols), *column_tables(rows), mirror_tables(rows)]))
    limit = pltpu.CompilerParams(vmem_limit_bytes=24 * 1024 * 1024)
    mixed, crossed = pl.pallas_call(
        spectrum_kernel,
        out_shape=(jax.ShapeDtypeStruct((rows, cols // 2), F32), jax.ShapeDtypeStruct((rows, cols // 4), F32)),
        in_specs=whole(1),
        out_specs=tuple(whole(2)),
        compiler_params=limit,
        cost_estimate=pl.CostEstimate(flops=2 * 10**9, bytes_accessed=10**6, transcendentals=0),
        name="spectrum",
    )(root_spectrum)
    left = passed_along(noise[:, block_cols - margin:], "tx", 1)
    right = passed_along(noise[:, :margin], "tx", -1)
    mid_far, mid_near = exchanged(noise, noise, "ty")
    left_far, left_near = exchanged(left, left, "ty")
    right_far, right_near = exchanged(right, right, "ty")
    strip = jax.ShapeDtypeStruct((margin, margin), F32)
    block = jax.ShapeDtypeStruct((margin, block_cols), F32)
    tall = jax.ShapeDtypeStruct((rows, block_cols), F32)
    even, odd = pl.pallas_call(
        rows_kernel,
        out_shape=(tall, tall),
        in_specs=whole(8),
        out_specs=tuple(whole(2)),
        compiler_params=limit,
        cost_estimate=pl.CostEstimate(flops=10**7, bytes_accessed=10**4, transcendentals=0),
        name="rows",
    )(mid_far, noise, mid_near, left_far, left, left_near, right, tables)
    mid_far, mid, mid_near, left_far, left_own, left_near, right_far, right, right_near = pl.pallas_call(
        filter_kernel,
        out_shape=(block,) * 3 + (strip,) * 6,
        in_specs=whole(7),
        out_specs=tuple(whole(9)),
        compiler_params=limit,
        cost_estimate=pl.CostEstimate(flops=4 * 10**9, bytes_accessed=10**7, transcendentals=0),
        name="filter",
    )(even, odd, right_far, right_near, mixed, crossed, tables)
    right_far, right_near = exchanged(right_far, right_near, "ty")
    left_far, left_near = exchanged(left_far, left_near, "ty")
    mid_far, mid_near = exchanged(mid_far, mid_near, "ty")
    left = passed_along(right + right_far + right_near, "tx", 1)
    right = passed_along(left_own + left_far + left_near, "tx", -1)
    mid = mid + mid_far + mid_near
    return mid + jnp.concatenate([left, right], axis=1)


def solution(mesh):
    placed = (P("ty", "tx"), P())
    return jax.shard_map(per_device, mesh=mesh, in_specs=placed, out_specs=P("ty", "tx"), check_vma=False)
```

```python
import math

import numpy as np
import jax
import jax.numpy as jnp
from jax import lax
from jax.experimental import pallas as pl
from jax.experimental.pallas import tpu as pltpu
from jax.sharding import PartitionSpec as P


F32 = jnp.float32
BF16 = jnp.bfloat16


def halves(table):
    high = table.astype(BF16)
    low = (table - high.astype(np.float64)).astype(BF16)
    return [high, low]


def row_tables(cols):
    half = cols // 2
    quarter = cols // 4
    c = np.arange(half)[:, None]
    m = np.arange(quarter)[None, :]
    sign = (1.0 - 2.0 * (np.arange(half) % 2))
    even = 2.0 * np.pi * ((2 * m * c) % cols) / cols
    odd = 2.0 * np.pi * (((2 * m + 1) * c) % cols) / cols
    even_sine = -np.sin(even)
    even_sine[:, 0] = sign
    forward_even = np.concatenate([np.cos(even), even_sine], axis=1)
    forward_odd = np.concatenate([np.cos(odd), -np.sin(odd)], axis=1)
    twice = np.full((half, 1), 2.0)
    twice[0] = 1.0
    twice[quarter] = 1.0
    back_even = forward_even.T * twice
    back_odd = forward_odd.T * 2.0
    return np.stack(halves(forward_even) + halves(forward_odd) + halves(back_even) + halves(back_odd))


def column_tables(rows):
    third = rows // 3
    q = np.arange(third)[:, None]
    s = np.arange(third)[None, :]
    forward = []
    back = []
    for p in range(3):
        angle = 2.0 * np.pi * (((3 * q + p) * s) % rows) / rows
        table = np.block([[np.cos(angle), np.sin(angle)], [-np.sin(angle), np.cos(angle)]])
        forward += halves(table)
        back += halves(table.T)
    return np.stack(forward), np.stack(back)


def mirror_tables(rows):
    third = rows // 3
    eye = np.eye(third)
    zero = np.zeros((third, third))
    same = eye[(-np.arange(third)) % third]
    swapped = eye[::-1]
    return np.stack([np.block([[m, zero], [zero, -m]]) for m in (same, swapped)]).astype(BF16)


def split(values):
    high = values.astype(BF16)
    return high, (values - high.astype(F32)).astype(BF16)


def dot(left, right):
    return jnp.dot(left, right, preferred_element_type=F32)


def by_table(values, high, low):
    first, second = split(values)
    return dot(first, high) + dot(second, high) + dot(first, low)


def spectrum_kernel(root_ref, mixed_ref, crossed_ref):
    rows, cols = root_ref.shape
    third = rows // 3
    half = cols // 2
    quarter = cols // 4
    root = root_ref[...]
    k = lax.broadcasted_iota(jnp.int32, (cols, half), 0)
    lane = lax.broadcasted_iota(jnp.int32, (cols, half), 1)
    wanted = jnp.where(lane < quarter, 2 * lane, 2 * (lane - quarter) + 1)
    mirrored = jnp.where(wanted == 0, 0, cols - wanted)
    first_lane = lane == 0
    share = jnp.where(first_lane, 0.5, 1.0)
    nyquist = jnp.logical_and(first_lane, k == half)
    pick = jnp.where(jnp.logical_or(k == wanted, nyquist), share, 0.0).astype(BF16)
    pick_mirrored = jnp.where(jnp.logical_or(k == mirrored, nyquist), share, 0.0).astype(BF16)
    high, low = split(root)
    chosen = dot(high, pick) + dot(low, pick)
    chosen_mirrored = dot(high, pick_mirrored) + dot(low, pick_mirrored)
    difference = 0.5 * (root[:, :quarter] - root[:, half:half + quarter])
    i = lax.broadcasted_iota(jnp.int32, (third, rows), 0)
    j = lax.broadcasted_iota(jnp.int32, (third, rows), 1)
    scale = 0.5 / (rows * cols)
    c_high, c_low = split(chosen)
    m_high, m_low = split(chosen_mirrored)
    d_high, d_low = split(difference)
    block_lane = lax.broadcasted_iota(jnp.int32, (third, quarter), 1)
    for p in range(3):
        source = 3 * i + p
        target = rows - source
        target = jnp.where(target == rows, 0, target)
        order = jnp.where(j == source, 1.0, 0.0).astype(BF16)
        order_mirrored = jnp.where(j == target, 1.0, 0.0).astype(BF16)
        both = jnp.where(j == source, 1.0, 0.0) + jnp.where(j == target, 1.0, 0.0)
        both = both.astype(BF16)
        mixed = dot(order, c_high) + dot(order, c_low) + dot(order_mirrored, m_high) + dot(order_mirrored, m_low)
        mixed_ref[p * third:(p + 1) * third, :] = mixed * scale
        crossed = dot(both, d_high) + dot(both, d_low)
        crossed_ref[p * third:(p + 1) * third, :] = jnp.where(block_lane == 0, crossed * scale, 0.0)


def twice(block):
    return jnp.concatenate([block, block], axis=0)


def thirds(block):
    third = block.shape[0] // 3
    quarter = block.shape[1] // 2
    return [
        (block[j * third:(j + 1) * third, :quarter], block[j * third:(j + 1) * third, quarter:]) for j in range(3)
    ]


def spread(block):
    (real_0, imag_0), (real_1, imag_1), (real_2, imag_2) = thirds(block)
    root_three = math.sqrt(3.0) / 2.0
    sum_real = real_1 + real_2
    sum_imag = imag_1 + imag_2
    gap_real = root_three * (real_1 - real_2)
    gap_imag = root_three * (imag_1 - imag_2)
    base_real = real_0 - 0.5 * sum_real
    base_imag = imag_0 - 0.5 * sum_imag
    return [
        jnp.concatenate([real_0 + sum_real, imag_0 + sum_imag], axis=0),
        jnp.concatenate([base_real + gap_imag, base_imag - gap_real], axis=0),
        jnp.concatenate([base_real - gap_imag, base_imag + gap_real], axis=0),
    ]


def gathered(classes):
    third = classes[0].shape[0] // 2
    real = [value[:third] for value in classes]
    imag = [value[third:] for value in classes]
    root_three = math.sqrt(3.0) / 2.0
    sum_real = real[1] + real[2]
    sum_imag = imag[1] + imag[2]
    gap_real = root_three * (real[1] - real[2])
    gap_imag = root_three * (imag[1] - imag[2])
    base_real = real[0] - 0.5 * sum_real
    base_imag = imag[0] - 0.5 * sum_imag
    blocks = (
        (real[0] + sum_real, imag[0] + sum_imag),
        (base_real - gap_imag, base_imag + gap_real),
        (base_real + gap_imag, base_imag - gap_real),
    )
    return jnp.concatenate([jnp.concatenate(block, axis=1) for block in blocks], axis=0)


def swapped(odd, first, second):
    return jnp.where(odd, second, first), jnp.where(odd, first, second)


def rows_kernel(mid_far, mid_own, mid_near, left_far, left_own, left_near, right_own, tables_ref, even_ref, odd_ref):
    quarter = mid_own.shape[1] // 2
    row_ref = tables_ref.at[:8]
    odd_row = lax.axis_index("ty") % 2 == 1
    mid_0, mid_2 = swapped(odd_row, mid_far[...], mid_near[...])
    left_0, left_2 = swapped(odd_row, left_far[...], left_near[...])
    evens = []
    odds = []
    for mid, left, right in ((mid_0, left_0, None), (mid_own[...], left_own[...], right_own[...]), (mid_2, left_2, None)):
        first = mid[:, :quarter]
        second = mid[:, quarter:]
        plus, minus = (first, first) if right is None else (first + right, first - right)
        evens.append(jnp.concatenate([left + second, plus], axis=1))
        odds.append(jnp.concatenate([left - second, minus], axis=1))
    even_ref[...] = by_table(jnp.concatenate(evens, axis=0), row_ref[0], row_ref[1])
    odd_ref[...] = by_table(jnp.concatenate(odds, axis=0), row_ref[2], row_ref[3])


def added(block, strips, high, low):
    third = block.shape[0] // 3
    quarter = strips[0].shape[1]
    high = high[quarter:]
    share = dot(jnp.concatenate(strips, axis=1), jnp.concatenate([high, high], axis=0)) + dot(strips[0], low[quarter:])
    return jnp.concatenate([block[:third] + share[:third], block[third:2 * third], block[2 * third:] + share[third:]], axis=0)


def filter_kernel(even_ref, odd_ref, right_far, right_near, mixed_ref, crossed_ref, tables_ref, mid_far_out, mid_own_out, mid_near_out, left_far_out, left_own_out, left_near_out,
                  right_far_out, right_own_out, right_near_out):
    third, half = mid_own_out.shape
    row_ref, forward_ref, back_ref, mirror_ref = (tables_ref.at[a:b] for a, b in ((0, 8), (8, 14), (14, 20), (20, 22)))
    quarter = half // 2
    odd_row = lax.axis_index("ty") % 2 == 1
    right = jnp.concatenate(swapped(odd_row, right_far[...], right_near[...]), axis=0)
    even = added(even_ref[...], split(right), row_ref[0], row_ref[1])
    odd = added(odd_ref[...], split(-right), row_ref[2], row_ref[3])
    even_inputs = [split(value) for value in spread(even)]
    even_main = [dot(forward_ref[2 * p], jnp.concatenate(even_inputs[p], axis=1)) for p in range(3)]
    odd_inputs = [split(value) for value in spread(odd)]
    even_spec = []
    odd_spec = []
    for p in range(3):
        odd_main = dot(forward_ref[2 * p], jnp.concatenate(odd_inputs[p], axis=1))
        rest = dot(forward_ref[2 * p + 1], jnp.concatenate([even_inputs[p][0], odd_inputs[p][0]], axis=1))
        even_spec.append(even_main[p][:, :quarter] + even_main[p][:, quarter:] + rest[:, :quarter])
        odd_spec.append(odd_main[:, :quarter] + odd_main[:, quarter:] + rest[:, quarter:])
    odd_parts = []
    for p in range(3):
        odd_parts.append(split(odd_spec[p] * twice(mixed_ref[p * third:(p + 1) * third, quarter:])))
    even_parts = []
    for p in range(3):
        flipped = dot(mirror_ref[min(p, 1)], jnp.concatenate(split(even_spec[(3 - p) % 3]), axis=1))
        flipped = flipped[:, :quarter] + flipped[:, quarter:]
        rows = slice(p * third, (p + 1) * third)
        filtered = even_spec[p] * twice(mixed_ref[rows, :quarter]) + flipped * twice(crossed_ref[rows, :])
        even_parts.append(split(filtered))
    odd_main = [dot(back_ref[2 * p], jnp.concatenate(odd_parts[p], axis=1)) for p in range(3)]
    odd_back = []
    rests = []
    for p in range(3):
        rest = dot(back_ref[2 * p + 1], jnp.concatenate([even_parts[p][0], odd_parts[p][0]], axis=1))
        odd_back.append(odd_main[p][:, :quarter] + odd_main[p][:, quarter:] + rest[:, quarter:])
        rests.append(rest[:, :quarter])
    even_back = []
    for p in range(3):
        main = dot(back_ref[2 * p], jnp.concatenate(even_parts[p], axis=1))
        even_back.append(main[:, :quarter] + main[:, quarter:] + rests[p])
    odd = by_table(gathered(odd_back), row_ref[6], row_ref[7])
    even = by_table(gathered(even_back), row_ref[4], row_ref[5])
    lane = lax.broadcasted_iota(jnp.int32, (1, half), 1).astype(F32)
    rising = (lane + 0.5) / half
    falling = 1.0 - rising
    row = lax.broadcasted_iota(jnp.int32, (third, 1), 0).astype(F32)
    mids = []
    lefts = []
    rights = []
    for j in range(3):
        knots = (row + 0.5) / third + j
        if j == 0:
            weight = 0.5 * knots * knots
        elif j == 1:
            weight = 0.5 * (-2.0 * knots * knots + 6.0 * knots - 3.0)
        else:
            weight = 0.5 * (3.0 - knots) * (3.0 - knots)
        rows = slice(j * third, (j + 1) * third)
        lower = (even[rows] + odd[rows]) * (weight * rising)
        upper = (even[rows] - odd[rows]) * (weight * falling)
        lefts.append(lower[:, :quarter])
        rights.append(upper[:, quarter:])
        mids.append(jnp.concatenate([lower[:, quarter:], upper[:, :quarter]], axis=1))
    left_own_out[...] = lefts[1]
    right_own_out[...] = rights[1]
    mid_own_out[...] = mids[1]
    left_far_out[...], left_near_out[...] = swapped(odd_row, lefts[0], lefts[2])
    right_far_out[...], right_near_out[...] = swapped(odd_row, rights[0], rights[2])
    mid_far_out[...], mid_near_out[...] = swapped(odd_row, mids[0], mids[2])


def whole(count):
    return [pl.BlockSpec(memory_space=pltpu.VMEM)] * count


def passed_along(shard, axis, by):
    count = lax.axis_size(axis)
    return lax.ppermute(shard, axis, [(i, (i + by) % count) for i in range(count)])


def exchanged(to_far, to_near, axis):
    count = lax.axis_size(axis)
    assert count % 2 == 0
    far = [(i, (i - 1 + 2 * (i % 2)) % count) for i in range(count)]
    near = [(i, (i + 1 - 2 * (i % 2)) % count) for i in range(count)]
    from_far = lax.ppermute(to_far, axis, far)
    from_near = lax.ppermute(to_near, axis, near)
    return from_far, from_near


def per_device(noise, root_spectrum):
    margin, block_cols = noise.shape
    rows, cols = root_spectrum.shape
    tables = jnp.asarray(np.concatenate([row_tables(cols), *column_tables(rows), mirror_tables(rows)]))
    limit = pltpu.CompilerParams(vmem_limit_bytes=24 * 1024 * 1024)
    mixed, crossed = pl.pallas_call(
        spectrum_kernel,
        out_shape=(jax.ShapeDtypeStruct((rows, cols // 2), F32), jax.ShapeDtypeStruct((rows, cols // 4), F32)),
        in_specs=whole(1),
        out_specs=tuple(whole(2)),
        compiler_params=limit,
        cost_estimate=pl.CostEstimate(flops=2 * 10**9, bytes_accessed=10**6, transcendentals=0),
        name="spectrum",
    )(root_spectrum)
    left = passed_along(noise[:, block_cols - margin:], "tx", 1)
    right = passed_along(noise[:, :margin], "tx", -1)
    mid_far, mid_near = exchanged(noise, noise, "ty")
    left_far, left_near = exchanged(left, left, "ty")
    right_far, right_near = exchanged(right, right, "ty")
    strip = jax.ShapeDtypeStruct((margin, margin), F32)
    block = jax.ShapeDtypeStruct((margin, block_cols), F32)
    tall = jax.ShapeDtypeStruct((rows, block_cols), F32)
    even, odd = pl.pallas_call(
        rows_kernel,
        out_shape=(tall, tall),
        in_specs=whole(8),
        out_specs=tuple(whole(2)),
        compiler_params=limit,
        cost_estimate=pl.CostEstimate(flops=10**7, bytes_accessed=10**4, transcendentals=0),
        name="rows",
    )(mid_far, noise, mid_near, left_far, left, left_near, right, tables)
    mid_far, mid, mid_near, left_far, left_own, left_near, right_far, right, right_near = pl.pallas_call(
        filter_kernel,
        out_shape=(block,) * 3 + (strip,) * 6,
        in_specs=whole(7),
        out_specs=tuple(whole(9)),
        compiler_params=limit,
        cost_estimate=pl.CostEstimate(flops=4 * 10**9, bytes_accessed=10**7, transcendentals=0),
        name="filter",
    )(even, odd, right_far, right_near, mixed, crossed, tables)
    right_far, right_near = exchanged(right_far, right_near, "ty")
    left_far, left_near = exchanged(left_far, left_near, "ty")
    mid_far, mid_near = exchanged(mid_far, mid_near, "ty")
    left = passed_along(right + right_far + right_near, "tx", 1)
    right = passed_along(left_own + left_far + left_near, "tx", -1)
    mid = mid + mid_far + mid_near
    return mid + jnp.concatenate([left, right], axis=1)


def solution(mesh):
    placed = (P("ty", "tx"), P())
    return jax.shard_map(per_device, mesh=mesh, in_specs=placed, out_specs=P("ty", "tx"), check_vma=False)
```
